256 devices in a mesh: dom: 64 (over x, z, core), ens: 4 (over y).
Axes of the slice: x: 4, y: 4, z: 8, core: 2. Of those that a mesh axis runs over, the one named last changes fastest.
Arguments:
- link_flow: float32 [64, 131072], P('ens', 'dom'), may hold values from 0.2 to 1
- free_time: float32 [131072], P('dom'), may hold values from 0.1 to 4
- capacity: float32 [131072], P('dom'), may hold values from 0.5 to 1.5
- demand: float32 [64, 64, 256], P('ens', 'dom'), may hold values from 0.05 to 0.3
- path_od: int32 [64, 1024], P('dom'), may hold values from 0 to 255, never falling along the last dimension, each value on 1 to 8 neighbouring positions
- send_blocks: int32 [64, 64, 4], P('dom'), may hold values from 0 to 15
- send_counts: int32 [64, 64], P('dom'), may hold values from 0 to 4, as said below
- tile_links: int32 [64, 64, 4, 4, 128], P('dom'), may hold values from -128 to 127
- tile_paths: int32 [64, 64, 4], P('dom'), may hold values from 0 to 7
Outputs:
- link_load: float32 [64, 131072], P('ens', 'dom')
- path_flow: float32 [64, 65536], P('ens', 'dom')
- mean_time: float32 [131072], P('dom')
The draws below stay inside these ranges and needn't reach their ends.
Inputs may be any that keep to these rules, and one draw needn't show every extreme that they name: `path_od`: each row holds non-decreasing pair ids; every id of 0 .. 255 names 1 to 8 paths of its row. `send_counts`: some path owner receives 4 live tiles from every link partition.
All inputs are finite; a program needn't handle non-finite values.
Results may differ from the reference program's by a relative error of at most 0.0003.
Values sent between devices are 32-bit elements; how exact they have to be, the bound alone decides.
No kernel may reach another device: no remote copies, remote signals or barrier semaphores. Data moves between devices by JAX's collectives and lax.ppermute only.
A program may use at most 64 MiB of HBM per device.

```python
import math
import jax
import jax.numpy as jnp
import numpy as np
from jax import lax

LINK_BLOCKS = 16
PATH_BLOCKS = 8
BLOCK = 128
CAP = 4
HOPS = 4
ITERS = 2
SCENARIOS = 64
LINKS = 131072
PATHS_DEV = 1024
OD_DEV = 256
N_DOM = 64


def draw_free_time(key, part):
    uniform_draw = jax.random.uniform(key, (LINKS,), jnp.float32)
    return jnp.exp(math.log(0.1) + uniform_draw * math.log(10.0)).astype(jnp.float32)


def draw_send_counts(key, part):
    first_key = jax.random.fold_in(key, 11)
    second_key = jax.random.fold_in(key, 23)
    baseline = jax.random.randint(first_key, (N_DOM, N_DOM), 0, CAP)
    crowded = jax.random.randint(second_key, (max(1, N_DOM // 16),), 0, N_DOM)
    crowded_mask = jnp.zeros((N_DOM,), jnp.int32).at[crowded].set(1)
    return jnp.where(crowded_mask[None, :] == 1, CAP, baseline).astype(jnp.int32)


def set_ends(entries, stream_key, low, high):
    longest = entries.shape.index(max(entries.shape))
    spots = []
    for shift in (0, 1):
        where = [jax.random.randint(jax.random.fold_in(stream_key, axis), (), 0, length) for axis, length in enumerate(entries.shape)]
        where[longest] = (where[longest] + shift) % entries.shape[longest]
        spots.append(tuple(where))
    return entries.at[spots[0]].set(low).at[spots[1]].set(high)


def block_scale(rng, extent, split, least, top_value):
    loudness = 1.0
    for position, blocks in split:
        steps = jax.random.uniform(jax.random.fold_in(jax.random.fold_in(rng, 6), position), (blocks,), jnp.float32, least / len(split), top_value / len(split))
        loudness = loudness * jnp.repeat(jnp.exp(steps), extent[position] // blocks).reshape((-1,) + (1,) * (len(extent) - 1 - position))
    return loudness


def length_profile(count, total, bound, lean):
    portions = [(1 << 20) // math.isqrt(rank ** lean) + 1 for rank in range(2, count + 1)]
    spare, given = total - bound - (count - 1), [1] * (count - 1)
    while spare > 0:
        candidates = [i for i in range(count - 1) if given[i] < bound]
        pool, remaining = sum([portions[i] for i in candidates]), spare
        for i in candidates:
            addition = min(bound - given[i], max(1, remaining * portions[i] // pool), spare)
            given[i] = given[i] + addition
            spare = spare - addition
    return np.array([bound] + given)


def ragged_sizes(stream_key, number_of, total, limit, slope):
    if number_of == 2:
        one = jax.random.randint(stream_key, (), max(1, total - limit), min(limit, total - 1) + 1)
        return jnp.stack([one, total - one])
    tallies = jnp.asarray(length_profile(number_of, total, limit, slope), jnp.int32)
    couples = (number_of - 1) // 2
    giver, sink = tallies[1:1 + 2 * couples:2], tallies[2:2 + 2 * couples:2]
    margin = jnp.minimum(giver - 1, limit - sink)
    shifted = jax.random.randint(jax.random.fold_in(stream_key, 1), (couples,), 0, 1 << 20) % (margin + 1)
    tallies = tallies.at[1:1 + 2 * couples:2].set(giver - shifted).at[2:2 + 2 * couples:2].set(sink + shifted)
    return tallies[jax.random.permutation(jax.random.fold_in(stream_key, 2), number_of)]


def setup_inputs(seed: int = 0) -> dict:
    key_of = jax.random.split(jax.random.key(seed), 10)
    link_flow = jnp.clip(jnp.exp(math.log(1.0) - 1.609438 * jax.random.uniform(key_of[0], (SCENARIOS, LINKS), jnp.float32) ** block_scale(key_of[0], (SCENARIOS, LINKS), ((0, 4), (1, 64)), -0.2, 0.2)), 0.2, 1.0)
    free_time = draw_free_time(jax.random.fold_in(key_of[9], 71), 0)
    capacity = jnp.clip(jnp.exp(math.log(1.5) - 1.0986123 * jax.random.uniform(key_of[2], (LINKS,), jnp.float32) ** block_scale(key_of[2], (LINKS,), ((0, 64),), -0.2, 0.2)), 0.5, 1.5)
    demand = jnp.clip(0.05 + 0.25 * jax.random.uniform(key_of[3], (SCENARIOS, N_DOM, OD_DEV), jnp.float32) ** block_scale(key_of[3], (SCENARIOS, N_DOM, OD_DEV), ((0, 4), (1, 64)), -0.2, 0.2), 0.05, 0.3)
    path_od = jax.vmap(lambda own: jnp.searchsorted(jnp.cumsum(ragged_sizes(own, OD_DEV, PATHS_DEV, 8, 1)), jnp.arange(PATHS_DEV), side="right"))(jax.random.split(key_of[4], N_DOM)).reshape((N_DOM, PATHS_DEV)).astype(jnp.int32)
    send_blocks = set_ends(jax.random.randint(key_of[5], (N_DOM, N_DOM, CAP), 0, LINK_BLOCKS), jax.random.fold_in(key_of[5], 1), 0, LINK_BLOCKS - 1).astype(jnp.int32)
    send_counts = draw_send_counts(jax.random.fold_in(key_of[9], 71), 0)
    tile_links = set_ends(jax.random.randint(key_of[7], (N_DOM, N_DOM, CAP, HOPS, BLOCK), 0 - BLOCK, BLOCK), jax.random.fold_in(key_of[7], 1), 0 - BLOCK, BLOCK - 1).astype(jnp.int32)
    tile_paths = set_ends(jax.random.randint(key_of[8], (N_DOM, N_DOM, CAP), 0, PATH_BLOCKS), jax.random.fold_in(key_of[8], 1), 0, PATH_BLOCKS - 1).astype(jnp.int32)
    return dict(link_flow=link_flow, free_time=free_time, capacity=capacity, demand=demand, path_od=path_od, send_blocks=send_blocks, send_counts=send_counts, tile_links=tile_links, tile_paths=tile_paths)


dispersion = 2.0


def bpr_times(current, free_time, capacity):
    loading = current / capacity
    square = loading * loading
    return free_time * (1.0 + 0.15 * square * square)


def link_path_incidence(link_rows):
    positions = jnp.arange(link_rows.shape[-1], dtype=jnp.int32)
    return jnp.sum((link_rows[:, :, None, :] == positions[None, None, :, None]).astype(jnp.float32), axis=1)


def logit_split(path_cost, anchor_dest, demands):
    pair_count = demands.shape[1]
    lowest = jnp.full((path_cost.shape[0], pair_count), jnp.inf, path_cost.dtype).at[:, anchor_dest].min(path_cost)
    weight = jnp.exp(-dispersion * (path_cost - lowest[:, anchor_dest]))
    weight_sum = jnp.zeros((path_cost.shape[0], pair_count), path_cost.dtype).at[:, anchor_dest].add(weight)
    return demands[:, anchor_dest] * weight / weight_sum[:, anchor_dest]


def reference(link_flow, free_time, capacity, demand, path_od, send_blocks, send_counts, tile_links, tile_paths):
    scenarios = link_flow.shape[0]
    tile_count = N_DOM * CAP
    slot_ids = jnp.arange(CAP, dtype=jnp.int32)
    live_mask = (slot_ids[None, None, :] < send_counts[:, :, None]).astype(jnp.float32)
    offsets = (jnp.arange(N_DOM, dtype=jnp.int32) * LINK_BLOCKS)[None, :, None]
    global_blocks = (jnp.transpose(send_blocks, (1, 0, 2)) + offsets).astype(jnp.int32).reshape(N_DOM, tile_count)
    live_owner = jnp.transpose(live_mask, (1, 0, 2)).reshape(N_DOM, tile_count)
    demand_owner = jnp.transpose(demand, (1, 0, 2))
    current = link_flow
    path_rows = None
    for iteration in range(ITERS):
        link_times = bpr_times(current, free_time, capacity).reshape(scenarios, N_DOM * LINK_BLOCKS, BLOCK)

        def owner_round(accumulated, payload):
            global_block, tile_live, link_rows, path_block, anchor_dest, demands = payload
            section_travel_times = jnp.take(link_times, global_block, axis=1) * tile_live[None, :, None]
            one_hot_selector = link_path_incidence(link_rows.reshape(tile_count, HOPS, BLOCK))
            partial_link_value = jnp.einsum("cbe,bek->bck", section_travel_times, one_hot_selector, precision=lax.Precision.HIGHEST)
            block_ids = path_block.reshape(tile_count)
            path_cost = jax.ops.segment_sum(partial_link_value, block_ids, num_segments=PATH_BLOCKS)
            path_cost = jnp.transpose(path_cost, (1, 0, 2)).reshape(scenarios, PATH_BLOCKS * BLOCK)
            path_flow = logit_split(path_cost, anchor_dest, demands)
            section_flow = jnp.take(path_flow.reshape(scenarios, PATH_BLOCKS, BLOCK), block_ids, axis=1)
            loaded_link_flow = jnp.einsum("mwa,wya->wmy", section_flow, one_hot_selector, precision=lax.Precision.HIGHEST)
            loaded_link_flow = loaded_link_flow * tile_live[:, None, None]
            return accumulated.at[global_block].add(loaded_link_flow), path_flow

        initial = jnp.zeros((N_DOM * LINK_BLOCKS, scenarios, BLOCK), jnp.float32)
        auxiliary, path_rows = lax.scan(owner_round, initial, (global_blocks, live_owner, tile_links, tile_paths, path_od, demand_owner))
        auxiliary = jnp.transpose(auxiliary, (1, 0, 2)).reshape(scenarios, N_DOM * LINK_BLOCKS * BLOCK)
        current = current + (auxiliary - current) / (iteration + 2.0)
    path_flow = jnp.transpose(path_rows, (1, 0, 2)).reshape(scenarios, N_DOM * PATH_BLOCKS * BLOCK)
    mean_time = jnp.sum(bpr_times(current, free_time, capacity), axis=0) / scenarios
    return current, path_flow, mean_time
```

```python
import functools
import jax
import jax.numpy as jnp
import numpy as np
from jax import lax
from jax.experimental import pallas as pl
from jax.experimental.pallas import tpu as pltpu
from jax.sharding import Mesh, PartitionSpec as P

ITERS = 2
NX, NZ, NC = 4, 8, 2
LB, PB, BLK, CAP, HOPS = 16, 8, 128, 4, 4
Q = 16
OWN = NZ
PART = NX * NC
TILES = OWN * PART * CAP
UNROLL = 8
SLOTS = TILES + UNROLL
ZERO_LINK = PART * LB
ZERO_PATH = OWN * PB
dispersion = 2.0


def bpr_times(current, free_time, capacity):
    loading = current / capacity
    square = loading * loading
    return free_time * (1.0 + 0.15 * square * square)


def split3(v):
    hi = v.astype(jnp.bfloat16)
    rest = v - hi.astype(jnp.float32)
    mid = rest.astype(jnp.bfloat16)
    low = (rest - mid.astype(jnp.float32)).astype(jnp.bfloat16)
    return jnp.concatenate([hi, mid, low], axis=0)


def incidence(hops):
    rows = [
        jnp.broadcast_to(hops[h : h + 1, :], (16, BLK)).astype(jnp.bfloat16) for h in range(HOPS)
    ]
    base = lax.broadcasted_iota(jnp.int32, (16, BLK), 0).astype(jnp.float32)
    one = jnp.ones((16, BLK), jnp.bfloat16)
    zero = jnp.zeros((16, BLK), jnp.bfloat16)
    chunks = []
    for i in range(BLK // 16):
        ids = (base + float(16 * i)).astype(jnp.bfloat16)
        hit = [jnp.where(r == ids, one, zero) for r in rows]
        chunks.append((hit[0] + hit[1]) + (hit[2] + hit[3]))
    return jnp.concatenate(chunks, axis=0)


def tile_kernel(count_ref, codes_ref, links_ref, *refs, ins, outs, forward):
    in_refs = refs[:ins]
    out_refs = refs[ins : ins + outs]
    parts, acc = refs[ins + outs :]
    in_blocks = (ZERO_LINK if forward else ZERO_PATH) // ins
    out_blocks = (ZERO_PATH if forward else ZERO_LINK) // outs
    for n, ref in enumerate(in_refs):

        def load(i, _, n=n, ref=ref):
            parts[n * in_blocks + i] = split3(ref[i])
            return 0

        lax.fori_loop(0, in_blocks, load, 0, unroll=4)
    parts[ins * in_blocks] = jnp.zeros(parts.shape[1:], parts.dtype)
    acc[...] = jnp.zeros_like(acc)

    def group(i, _):
        results = []
        for u in range(UNROLL):
            code = codes_ref[i * UNROLL + u]
            tile = code & 255
            link = (code >> 8) & 255
            path = code >> 16
            e = incidence(links_ref[tile])
            if forward:
                r = jnp.dot(parts[link], e, preferred_element_type=jnp.float32)
            else:
                r = lax.dot_general(
                    parts[path], e, (((1,), (1,)), ((), ())), preferred_element_type=jnp.float32
                )
            results.append((path if forward else link, r[:Q] + r[Q : 2 * Q] + r[2 * Q :]))
        for where, r in results:
            acc[where] += r
        return 0

    lax.fori_loop(0, (count_ref[0] + UNROLL - 1) // UNROLL, group, 0)
    for n, ref in enumerate(out_refs):

        def store(i, _, n=n, ref=ref):
            ref[i] = acc[n * out_blocks + i]
            return 0

        lax.fori_loop(0, out_blocks, store, 0, unroll=4)


def tile_call(count, codes, links, arrays, outs, forward):
    in_n, out_n = (ZERO_LINK, ZERO_PATH) if forward else (ZERO_PATH, ZERO_LINK)
    shape = jax.ShapeDtypeStruct((out_n // outs, Q, BLK), jnp.float32)
    smem = pl.BlockSpec(memory_space=pltpu.SMEM)
    vmem = pl.BlockSpec(memory_space=pltpu.VMEM)
    return pl.pallas_call(
        functools.partial(tile_kernel, ins=len(arrays), outs=outs, forward=forward),
        out_shape=[shape] * outs,
        in_specs=[smem, smem, vmem] + [vmem] * len(arrays),
        out_specs=[vmem] * outs,
        scratch_shapes=[
            pltpu.VMEM((in_n + 1, 3 * Q, BLK), jnp.bfloat16),
            pltpu.VMEM((out_n + 1, Q, BLK), jnp.float32),
        ],
        name="tile_costs" if forward else "tile_loads",
    )(count, codes, links, *arrays)


def logit_kernel(od_ref, demand_ref, *refs):
    partials, (flow_ref, wide_ref) = refs[:NZ], refs[NZ:]
    width = PB * BLK
    blocks = []
    for b in range(PB):
        terms = [p[b] for p in partials]
        while len(terms) > 1:
            terms = [terms[i] + terms[i + 1] for i in range(0, len(terms), 2)]
        blocks.append(terms[0])
    cost = jnp.concatenate(blocks, axis=1)
    od = jnp.broadcast_to(od_ref[...], (Q, width))
    lane = lax.broadcasted_iota(jnp.int32, (Q, width), 1)
    back = {s: (pltpu.roll(od, s, 1) == od) & (lane >= s) for s in (1, 2, 4)}
    ahead = {s: (pltpu.roll(od, width - s, 1) == od) & (lane < width - s) for s in (1, 2, 4)}

    def from_last(v):
        for s in (1, 2, 4):
            v = jnp.where(ahead[s], pltpu.roll(v, width - s, 1), v)
        return v

    low = cost
    for s in (1, 2, 4):
        low = jnp.where(back[s], jnp.minimum(low, pltpu.roll(low, s, 1)), low)
    weight = jnp.exp(-dispersion * (cost - from_last(low)))
    total = weight
    for s in (1, 2, 4):
        total = jnp.where(back[s], total + pltpu.roll(total, s, 1), total)
    total = from_last(total)
    pairs = demand_ref.shape[1]
    pick = (
        lax.broadcasted_iota(jnp.int32, (pairs, width), 0)
        == jnp.broadcast_to(od_ref[...], (pairs, width))
    ).astype(jnp.float32).astype(jnp.bfloat16)
    d = jnp.dot(split3(demand_ref[...]), pick, preferred_element_type=jnp.float32)
    d = d[:Q] + d[Q : 2 * Q] + d[2 * Q :]
    flow = d * weight / total
    wide_ref[...] = flow
    for b in range(PB):
        flow_ref[b] = flow[:, b * BLK : (b + 1) * BLK]


def logit_call(od, demand, partials):
    return pl.pallas_call(
        logit_kernel,
        out_shape=[
            jax.ShapeDtypeStruct((PB, Q, BLK), jnp.float32),
            jax.ShapeDtypeStruct((Q, PB * BLK), jnp.float32),
        ],
        name="logit",
    )(od, demand, *partials)


def shift(v, axis, size, by):
    return lax.ppermute(v, axis, [(i, (i + by) % size) for i in range(size)])


def live_list(info, tile_paths, x, z, c):
    blocks = info[:, : NX * NZ * NC * CAP].reshape(NC, NX, NX, NZ, NC, CAP)
    counts = info[:, NX * NZ * NC * CAP : NX * NZ * NC * (CAP + 1)].reshape(NC, NX, NX, NZ, NC)
    blocks = lax.dynamic_slice(blocks, (0, 0, x, 0, c, 0), (NC, NX, 1, NZ, 1, CAP))
    counts = lax.dynamic_slice(counts, (0, 0, x, 0, c), (NC, NX, 1, NZ, 1))
    blocks = blocks.reshape(NC, NX, NZ, CAP)
    counts = counts.reshape(NC, NX, NZ, 1)
    shape = (NC, NX, NZ, CAP)
    dc, dx, zo, k = (lax.broadcasted_iota(jnp.int32, shape, i) for i in range(4))
    xs, cs = (x - dx) % NX, c ^ dc
    tile = zo * (PART * CAP) + xs * (NC * CAP) + cs * CAP + k
    link = (dc * NX + dx) * LB + blocks
    ordered = tile_paths.reshape(1, TILES)
    tile = tile.reshape(TILES, 1)
    positions = lax.broadcasted_iota(jnp.int32, (TILES, TILES), 1)
    paths = jnp.sum(jnp.where(positions == tile, ordered, 0), axis=1, keepdims=True)
    path = ((zo - z) % NZ).reshape(TILES, 1) * PB + paths
    live = (k < counts).reshape(TILES)
    pad = ZERO_LINK * 256 + ZERO_PATH * 65536
    code = tile + link.reshape(TILES, 1) * 256 + path * 65536 - pad
    before = positions < lax.broadcasted_iota(jnp.int32, (TILES, TILES), 0)
    rank = jnp.sum(jnp.where(before & live[None, :], 1, 0), axis=1, keepdims=True)
    target = lax.broadcasted_iota(jnp.int32, (TILES, SLOTS), 1)
    hit = (rank == target) & live[:, None]
    codes = jnp.sum(jnp.where(hit, code, 0), axis=0) + pad
    return jnp.sum(live.astype(jnp.int32)).reshape(1), codes


def local(
    link_flow,
    free_time,
    capacity,
    demand,
    path_od,
    send_blocks,
    send_counts,
    tile_links,
    tile_paths,
):
    x, z, c = lax.axis_index("x"), lax.axis_index("z"), lax.axis_index("c")
    rows = PART * CAP * HOPS
    links = tile_links[0].reshape(NX, NZ, NC * CAP * HOPS, BLK)
    links = jnp.transpose(links, (1, 0, 2, 3)).reshape(NZ, rows, BLK)
    paths = tile_paths[0].reshape(NX, NZ, NC * CAP)
    paths = jnp.transpose(paths, (1, 0, 2)).reshape(NZ, 1, PART * CAP)
    paths = jnp.pad(paths, ((0, 0), (0, 7), (0, BLK - PART * CAP)))
    payload = jnp.concatenate([links, paths], axis=1)
    payload = lax.all_to_all(payload, "z", split_axis=0, concat_axis=0, tiled=True)
    tiles = payload[:, :rows].reshape(TILES, HOPS, BLK).astype(jnp.float32)
    owner_paths = payload[:, rows, : PART * CAP]

    info = jnp.concatenate([send_blocks[0].reshape(-1), send_counts[0].reshape(-1)])
    info = info.astype(jnp.float32)
    info_size = info.shape[0]
    info = jnp.pad(info, (0, Q * BLK - info_size)).reshape(1, Q, BLK)
    free = free_time.reshape(LB, 1, BLK)
    room = capacity.reshape(LB, 1, BLK)
    current = jnp.transpose(link_flow.reshape(Q, LB, BLK), (1, 0, 2))
    od = path_od
    demands = demand[:, 0, :]
    count = codes = wide = None
    for iteration in range(ITERS):
        times = bpr_times(current, free, room)
        if iteration == 0:
            times = jnp.concatenate([times, info], axis=0)
        mine = [times] + [shift(times, "x", NX, d) for d in range(1, NX)]
        other = [shift(m, "c", NC, 1) for m in mine]
        gathered = mine + other
        if iteration == 0:
            infos = jnp.stack([g[LB].reshape(-1)[:info_size] for g in gathered])
            count, codes = live_list(infos.astype(jnp.int32), owner_paths, x, z, c)
        partials = tile_call(count, codes, tiles, gathered, NZ, True)
        partials = [partials[0]] + [shift(partials[d], "z", NZ, d) for d in range(1, NZ)]
        flow, wide = logit_call(od, demands, partials)
        flows = [flow] + [shift(flow, "z", NZ, -d) for d in range(1, NZ)]
        loads = tile_call(count, codes, tiles, flows, PART, False)
        sums = [loads[d] + shift(loads[NX + d], "c", NC, 1) for d in range(NX)]
        auxiliary = sums[0]
        for d in range(1, NX):
            auxiliary = auxiliary + shift(sums[d], "x", NX, -d)
        current = current + (auxiliary - current) / (iteration + 2.0)
    final_times = jnp.sum(bpr_times(current, free, room), axis=1).reshape(LB * BLK)
    mean_time = lax.psum(final_times, "ens") / (Q * lax.axis_size("ens"))
    return (jnp.transpose(current, (1, 0, 2)).reshape(Q, LB * BLK), wide, mean_time)


def solution(mesh):
    fine = Mesh(
        np.asarray(mesh.devices).reshape(NX, NZ, NC, -1), ("x", "z", "c", "ens")
    )
    dom = ("x", "z", "c")
    in_specs = (
        P("ens", dom),
        P(dom),
        P(dom),
        P("ens", dom, None),
        P(dom, None),
        P(dom, None, None),
        P(dom, None),
        P(dom, None, None, None, None),
        P(dom, None, None),
    )
    out_specs = (P("ens", dom), P("ens", dom), P(dom))
    return jax.shard_map(local, mesh=fine, in_specs=in_specs, out_specs=out_specs, check_vma=False)
```

```python
import functools
import jax
import jax.numpy as jnp
import numpy as np
from jax import lax
from jax.experimental import pallas as pl
from jax.experimental.pallas import tpu as pltpu
from jax.sharding import Mesh, PartitionSpec as P

ITERS = 2
NX, NZ, NC = 4, 8, 2
LB, PB, BLK, CAP, HOPS = 16, 8, 128, 4, 4
Q = 16
OWN = NZ
PART = NX * NC
TILES = OWN * PART * CAP
UNROLL = 8
SLOTS = TILES + UNROLL
ZERO_LINK = PART * LB
ZERO_PATH = OWN * PB
dispersion = 2.0


def bpr_times(current, free_time, capacity):
    loading = current / capacity
    square = loading * loading
    return free_time * (1.0 + 0.15 * square * square)


def split3(v):
    hi = v.astype(jnp.bfloat16)
    rest = v - hi.astype(jnp.float32)
    mid = rest.astype(jnp.bfloat16)
    low = (rest - mid.astype(jnp.float32)).astype(jnp.bfloat16)
    return jnp.concatenate([hi, mid, low], axis=0)


def incidence(hops):
    rows = [
        jnp.broadcast_to(hops[h : h + 1, :], (16, BLK)).astype(jnp.bfloat16) for h in range(HOPS)
    ]
    base = lax.broadcasted_iota(jnp.int32, (16, BLK), 0).astype(jnp.float32)
    one = jnp.ones((16, BLK), jnp.bfloat16)
    zero = jnp.zeros((16, BLK), jnp.bfloat16)
    chunks = []
    for i in range(BLK // 16):
        ids = (base + float(16 * i)).astype(jnp.bfloat16)
        hit = [jnp.where(r == ids, one, zero) for r in rows]
        chunks.append((hit[0] + hit[1]) + (hit[2] + hit[3]))
    return jnp.concatenate(chunks, axis=0)


def tile_kernel(count_ref, codes_ref, links_ref, *refs, ins, outs, forward):
    in_refs = refs[:ins]
    out_refs = refs[ins : ins + outs]
    parts, acc = refs[ins + outs :]
    in_blocks = (ZERO_LINK if forward else ZERO_PATH) // ins
    out_blocks = (ZERO_PATH if forward else ZERO_LINK) // outs
    for n, ref in enumerate(in_refs):

        def load(i, _, n=n, ref=ref):
            parts[n * in_blocks + i] = split3(ref[i])
            return 0

        lax.fori_loop(0, in_blocks, load, 0, unroll=4)
    parts[ins * in_blocks] = jnp.zeros(parts.shape[1:], parts.dtype)
    acc[...] = jnp.zeros_like(acc)

    def group(i, _):
        results = []
        for u in range(UNROLL):
            code = codes_ref[i * UNROLL + u]
            tile = code & 255
            link = (code >> 8) & 255
            path = code >> 16
            e = incidence(links_ref[tile])
            if forward:
                r = jnp.dot(parts[link], e, preferred_element_type=jnp.float32)
            else:
                r = lax.dot_general(
                    parts[path], e, (((1,), (1,)), ((), ())), preferred_element_type=jnp.float32
                )
            results.append((path if forward else link, r[:Q] + r[Q : 2 * Q] + r[2 * Q :]))
        for where, r in results:
            acc[where] += r
        return 0

    lax.fori_loop(0, (count_ref[0] + UNROLL - 1) // UNROLL, group, 0)
    for n, ref in enumerate(out_refs):

        def store(i, _, n=n, ref=ref):
            ref[i] = acc[n * out_blocks + i]
            return 0

        lax.fori_loop(0, out_blocks, store, 0, unroll=4)


def tile_call(count, codes, links, arrays, outs, forward):
    in_n, out_n = (ZERO_LINK, ZERO_PATH) if forward else (ZERO_PATH, ZERO_LINK)
    shape = pltpu.VMEM((out_n // outs, Q, BLK), jnp.float32)
    arrays = [pltpu.with_memory_space_constraint(a, pltpu.VMEM) for a in arrays]
    links = pltpu.with_memory_space_constraint(links, pltpu.VMEM)
    smem = pl.BlockSpec(memory_space=pltpu.SMEM)
    vmem = pl.BlockSpec(memory_space=pltpu.VMEM)
    return pl.pallas_call(
        functools.partial(tile_kernel, ins=len(arrays), outs=outs, forward=forward),
        out_shape=[shape] * outs,
        in_specs=[smem, smem, vmem] + [vmem] * len(arrays),
        out_specs=[vmem] * outs,
        scratch_shapes=[
            pltpu.VMEM((in_n + 1, 3 * Q, BLK), jnp.bfloat16),
            pltpu.VMEM((out_n + 1, Q, BLK), jnp.float32),
        ],
        name="tile_costs" if forward else "tile_loads",
    )(count, codes, links, *arrays)


def logit_kernel(od_ref, demand_ref, *refs):
    partials, (flow_ref, wide_ref) = refs[:NZ], refs[NZ:]
    width = PB * BLK
    blocks = []
    for b in range(PB):
        terms = [p[b] for p in partials]
        while len(terms) > 1:
            terms = [terms[i] + terms[i + 1] for i in range(0, len(terms), 2)]
        blocks.append(terms[0])
    cost = jnp.concatenate(blocks, axis=1)
    od = jnp.broadcast_to(od_ref[...], (Q, width))
    lane = lax.broadcasted_iota(jnp.int32, (Q, width), 1)
    back = {s: (pltpu.roll(od, s, 1) == od) & (lane >= s) for s in (1, 2, 4)}
    ahead = {s: (pltpu.roll(od, width - s, 1) == od) & (lane < width - s) for s in (1, 2, 4)}

    def from_last(v):
        for s in (1, 2, 4):
            v = jnp.where(ahead[s], pltpu.roll(v, width - s, 1), v)
        return v

    low = cost
    for s in (1, 2, 4):
        low = jnp.where(back[s], jnp.minimum(low, pltpu.roll(low, s, 1)), low)
    weight = jnp.exp(-dispersion * (cost - from_last(low)))
    total = weight
    for s in (1, 2, 4):
        total = jnp.where(back[s], total + pltpu.roll(total, s, 1), total)
    total = from_last(total)
    pairs = demand_ref.shape[1]
    pick = (
        lax.broadcasted_iota(jnp.int32, (pairs, width), 0)
        == jnp.broadcast_to(od_ref[...], (pairs, width))
    ).astype(jnp.float32).astype(jnp.bfloat16)
    d = jnp.dot(split3(demand_ref[...]), pick, preferred_element_type=jnp.float32)
    d = d[:Q] + d[Q : 2 * Q] + d[2 * Q :]
    flow = d * weight / total
    wide_ref[...] = flow
    for b in range(PB):
        flow_ref[b] = flow[:, b * BLK : (b + 1) * BLK]


def logit_call(od, demand, partials):
    partials = [pltpu.with_memory_space_constraint(p, pltpu.VMEM) for p in partials]
    vmem = pl.BlockSpec(memory_space=pltpu.VMEM)
    return pl.pallas_call(
        logit_kernel,
        out_shape=[
            pltpu.VMEM((PB, Q, BLK), jnp.float32),
            jax.ShapeDtypeStruct((Q, PB * BLK), jnp.float32),
        ],
        in_specs=[vmem] * (2 + NZ),
        out_specs=[vmem, vmem],
        name="logit",
    )(od, demand, *partials)


def shift(v, axis, size, by):
    return lax.ppermute(v, axis, [(i, (i + by) % size) for i in range(size)])


def live_list(info, tile_paths, x, z, c):
    blocks = info[:, : NX * NZ * NC * CAP].reshape(NC, NX, NX, NZ, NC, CAP)
    counts = info[:, NX * NZ * NC * CAP : NX * NZ * NC * (CAP + 1)].reshape(NC, NX, NX, NZ, NC)
    blocks = lax.dynamic_slice(blocks, (0, 0, x, 0, c, 0), (NC, NX, 1, NZ, 1, CAP))
    counts = lax.dynamic_slice(counts, (0, 0, x, 0, c), (NC, NX, 1, NZ, 1))
    blocks = blocks.reshape(NC, NX, NZ, CAP)
    counts = counts.reshape(NC, NX, NZ, 1)
    shape = (NC, NX, NZ, CAP)
    dc, dx, zo, k = (lax.broadcasted_iota(jnp.int32, shape, i) for i in range(4))
    xs, cs = (x - dx) % NX, c ^ dc
    tile = zo * (PART * CAP) + xs * (NC * CAP) + cs * CAP + k
    link = (dc * NX + dx) * LB + blocks
    ordered = tile_paths.reshape(1, TILES)
    tile = tile.reshape(TILES, 1)
    positions = lax.broadcasted_iota(jnp.int32, (TILES, TILES), 1)
    paths = jnp.sum(jnp.where(positions == tile, ordered, 0), axis=1, keepdims=True)
    path = ((zo - z) % NZ).reshape(TILES, 1) * PB + paths
    live = (k < counts).reshape(TILES)
    pad = ZERO_LINK * 256 + ZERO_PATH * 65536
    code = tile + link.reshape(TILES, 1) * 256 + path * 65536 - pad
    before = positions < lax.broadcasted_iota(jnp.int32, (TILES, TILES), 0)
    rank = jnp.sum(jnp.where(before & live[None, :], 1, 0), axis=1, keepdims=True)
    target = lax.broadcasted_iota(jnp.int32, (TILES, SLOTS), 1)
    hit = (rank == target) & live[:, None]
    codes = jnp.sum(jnp.where(hit, code, 0), axis=0) + pad
    return jnp.sum(live.astype(jnp.int32)).reshape(1), codes


def body(
    link_flow,
    free_time,
    capacity,
    demand,
    path_od,
    send_blocks,
    send_counts,
    tile_links,
    tile_paths,
):
    x, z, c = lax.axis_index("x"), lax.axis_index("z"), lax.axis_index("c")
    rows = PART * CAP * HOPS
    links = tile_links[0].reshape(NX, NZ, NC * CAP * HOPS, BLK)
    links = jnp.transpose(links, (1, 0, 2, 3)).reshape(NZ, rows, BLK)
    paths = tile_paths[0].reshape(NX, NZ, NC * CAP)
    paths = jnp.transpose(paths, (1, 0, 2)).reshape(NZ, 1, PART * CAP)
    paths = jnp.pad(paths, ((0, 0), (0, 7), (0, BLK - PART * CAP)))
    payload = jnp.concatenate([links, paths], axis=1)
    payload = lax.all_to_all(payload, "z", split_axis=0, concat_axis=0, tiled=True)
    tiles = payload[:, :rows].reshape(TILES, HOPS, BLK).astype(jnp.float32)
    owner_paths = payload[:, rows, : PART * CAP]

    info = jnp.concatenate([send_blocks[0].reshape(-1), send_counts[0].reshape(-1)])
    info = info.astype(jnp.float32)
    info_size = info.shape[0]
    info = jnp.pad(info, (0, Q * BLK - info_size)).reshape(1, Q, BLK)
    free = free_time.reshape(LB, 1, BLK)
    room = capacity.reshape(LB, 1, BLK)
    current = jnp.transpose(link_flow.reshape(Q, LB, BLK), (1, 0, 2))
    od = path_od
    demands = demand[:, 0, :]
    count = codes = wide = None
    for iteration in range(ITERS):
        times = bpr_times(current, free, room)
        if iteration == 0:
            times = jnp.concatenate([times, info], axis=0)
        mine = [times] + [shift(times, "x", NX, d) for d in range(1, NX)]
        other = [shift(m, "c", NC, 1) for m in mine]
        gathered = mine + other
        if iteration == 0:
            infos = jnp.stack([g[LB].reshape(-1)[:info_size] for g in gathered])
            count, codes = live_list(infos.astype(jnp.int32), owner_paths, x, z, c)
        partials = tile_call(count, codes, tiles, gathered, NZ, True)
        partials = [partials[0]] + [shift(partials[d], "z", NZ, d) for d in range(1, NZ)]
        flow, wide = logit_call(od, demands, partials)
        flows = [flow] + [shift(flow, "z", NZ, -d) for d in range(1, NZ)]
        loads = tile_call(count, codes, tiles, flows, PART, False)
        sums = [loads[d] + shift(loads[NX + d], "c", NC, 1) for d in range(NX)]
        auxiliary = sums[0]
        for d in range(1, NX):
            auxiliary = auxiliary + shift(sums[d], "x", NX, -d)
        current = current + (auxiliary - current) / (iteration + 2.0)
    final_times = jnp.sum(bpr_times(current, free, room), axis=1).reshape(LB * BLK)
    groups = lax.axis_size("ens")
    final_times = final_times.reshape(LB, BLK)
    total = final_times
    for d in range(1, groups):
        total = total + shift(final_times, "ens", groups, d)
    mean_time = total.reshape(LB * BLK) / (Q * groups)
    return (jnp.transpose(current, (1, 0, 2)).reshape(Q, LB * BLK), wide, mean_time)


def solution(mesh):
    fine = Mesh(
        np.asarray(mesh.devices).reshape(NX, NZ, NC, -1), ("x", "z", "c", "ens")
    )
    dom = ("x", "z", "c")
    in_specs = (
        P("ens", dom),
        P(dom),
        P(dom),
        P("ens", dom, None),
        P(dom, None),
        P(dom, None, None),
        P(dom, None),
        P(dom, None, None, None, None),
        P(dom, None, None),
    )
    out_specs = (P("ens", dom), P("ens", dom), P(dom))
    return jax.shard_map(body, mesh=fine, in_specs=in_specs, out_specs=out_specs, check_vma=False)
```

```python
import functools
import jax
import jax.numpy as jnp
import numpy as np
from jax import lax
from jax.experimental import pallas as pl
from jax.experimental.pallas import tpu as pltpu
from jax.sharding import Mesh, PartitionSpec as P

ITERS = 2
NX, NZ, NC = 4, 8, 2
LB, PB, BLK, CAP, HOPS = 16, 8, 128, 4, 4
Q = 16
OWN = NZ
PART = NX * NC
TILES = OWN * PART * CAP
UNROLL = 16
SLOTS = TILES + UNROLL
ZERO_LINK = PART * LB
ZERO_PATH = OWN * PB
dispersion = 2.0


def bpr_times(current, free_time, capacity):
    loading = current / capacity
    square = loading * loading
    return free_time * (1.0 + 0.15 * square * square)


def split3(v):
    hi = v.astype(jnp.bfloat16)
    rest = v - hi.astype(jnp.float32)
    mid = rest.astype(jnp.bfloat16)
    low = (rest - mid.astype(jnp.float32)).astype(jnp.bfloat16)
    return jnp.concatenate([hi, mid, low], axis=0)


def incidence(hops):
    rows = [
        jnp.broadcast_to(hops[h : h + 1, :], (16, BLK)).astype(jnp.bfloat16) for h in range(HOPS)
    ]
    base = lax.broadcasted_iota(jnp.int32, (16, BLK), 0).astype(jnp.float32)
    one = jnp.ones((16, BLK), jnp.bfloat16)
    zero = jnp.zeros((16, BLK), jnp.bfloat16)
    chunks = []
    for i in range(BLK // 16):
        ids = (base + float(16 * i)).astype(jnp.bfloat16)
        hit = [jnp.where(r == ids, one, zero) for r in rows]
        chunks.append((hit[0] + hit[1]) + (hit[2] + hit[3]))
    return jnp.concatenate(chunks, axis=0)


def tile_kernel(
    count_ref, codes_ref, names_ref, links_ref, *refs, ins, outs, forward, segments
):
    in_refs = refs[:ins]
    out_refs = refs[ins : ins + outs]
    parts, acc = refs[ins + outs :]
    filled = 0
    for n, first, blocks in segments:

        def load(i, _, ref=in_refs[n], first=first, filled=filled):
            parts[filled + i] = split3(ref[first + i])
            return 0

        lax.fori_loop(0, blocks, load, 0, unroll=4)
        filled += blocks
    parts[filled] = jnp.zeros(parts.shape[1:], parts.dtype)
    acc[...] = jnp.zeros_like(acc)

    def group(i, _):
        results = []
        for u in range(UNROLL):
            code = codes_ref[i * UNROLL + u]
            tile = code & 511
            link = code >> 9
            path = names_ref[tile]
            e = incidence(links_ref[tile & 255])
            if forward:
                r = jnp.dot(parts[link], e, preferred_element_type=jnp.float32)
            else:
                r = lax.dot_general(
                    parts[path], e, (((1,), (1,)), ((), ())), preferred_element_type=jnp.float32
                )
            results.append((path if forward else link, r[:Q] + r[Q : 2 * Q] + r[2 * Q :]))
        for where, r in results:
            acc[where] += r
        return 0

    lax.fori_loop(0, (count_ref[0] + UNROLL - 1) // UNROLL, group, 0)
    stored = 0
    for ref in out_refs:

        def store(i, _, ref=ref, stored=stored):
            ref[i] = acc[stored + i]
            return 0

        lax.fori_loop(0, ref.shape[0], store, 0, unroll=4)
        stored += ref.shape[0]


def tile_call(count, codes, names, links, arrays, segments, sizes, forward):
    in_n, out_n = (ZERO_LINK, ZERO_PATH) if forward else (ZERO_PATH, ZERO_LINK)
    arrays = [pltpu.with_memory_space_constraint(a, pltpu.VMEM) for a in arrays]
    links = pltpu.with_memory_space_constraint(links, pltpu.VMEM)
    smem = pl.BlockSpec(memory_space=pltpu.SMEM)
    vmem = pl.BlockSpec(memory_space=pltpu.VMEM)
    return pl.pallas_call(
        functools.partial(
            tile_kernel,
            ins=len(arrays),
            outs=len(sizes),
            forward=forward,
            segments=segments,
        ),
        out_shape=[pltpu.VMEM((n, Q, BLK), jnp.float32) for n in sizes],
        in_specs=[smem, smem, smem, vmem] + [vmem] * len(arrays),
        out_specs=[vmem] * len(sizes),
        scratch_shapes=[
            pltpu.VMEM((in_n + 1, 3 * Q, BLK), jnp.bfloat16),
            pltpu.VMEM((out_n + 1, Q, BLK), jnp.float32),
        ],
        name="tile_costs" if forward else "tile_loads",
    )(count, codes, names, links, *arrays)


def logit_kernel(od_ref, demand_ref, *refs):
    partials, (flow_ref, wide_ref) = refs[:NZ], refs[NZ:]
    width = PB * BLK
    blocks = []
    for b in range(PB):
        terms = [p[b] for p in partials]
        while len(terms) > 1:
            terms = [terms[i] + terms[i + 1] for i in range(0, len(terms), 2)]
        blocks.append(terms[0])
    cost = jnp.concatenate(blocks, axis=1)
    od = jnp.broadcast_to(od_ref[...], (Q, width))
    lane = lax.broadcasted_iota(jnp.int32, (Q, width), 1)
    back = {s: (pltpu.roll(od, s, 1) == od) & (lane >= s) for s in (1, 2, 4)}
    ahead = {s: (pltpu.roll(od, width - s, 1) == od) & (lane < width - s) for s in (1, 2, 4)}

    def from_last(v):
        for s in (1, 2, 4):
            v = jnp.where(ahead[s], pltpu.roll(v, width - s, 1), v)
        return v

    low = cost
    for s in (1, 2, 4):
        low = jnp.where(back[s], jnp.minimum(low, pltpu.roll(low, s, 1)), low)
    weight = jnp.exp(-dispersion * (cost - from_last(low)))
    total = weight
    for s in (1, 2, 4):
        total = jnp.where(back[s], total + pltpu.roll(total, s, 1), total)
    total = from_last(total)
    pairs = demand_ref.shape[1]
    pick = (
        lax.broadcasted_iota(jnp.int32, (pairs, width), 0)
        == jnp.broadcast_to(od_ref[...], (pairs, width))
    ).astype(jnp.float32).astype(jnp.bfloat16)
    d = jnp.dot(split3(demand_ref[...]), pick, preferred_element_type=jnp.float32)
    d = d[:Q] + d[Q : 2 * Q] + d[2 * Q :]
    flow = d * weight / total
    wide_ref[...] = flow
    for b in range(PB):
        flow_ref[b] = flow[:, b * BLK : (b + 1) * BLK]


def logit_call(od, demand, partials):
    partials = [pltpu.with_memory_space_constraint(p, pltpu.VMEM) for p in partials]
    vmem = pl.BlockSpec(memory_space=pltpu.VMEM)
    return pl.pallas_call(
        logit_kernel,
        out_shape=[
            pltpu.VMEM((PB, Q, BLK), jnp.float32),
            jax.ShapeDtypeStruct((Q, PB * BLK), jnp.float32),
        ],
        in_specs=[vmem] * (2 + NZ),
        out_specs=[vmem, vmem],
        name="logit",
    )(od, demand, *partials)


def shift(v, axis, size, by):
    return lax.ppermute(v, axis, [(i, (i + by) % size) for i in range(size)])


def live_list(info, x, c):
    blocks = info[:, : NX * NZ * NC * CAP].reshape(NC, NX, NX, NZ, NC, CAP)
    counts = info[:, NX * NZ * NC * CAP : NX * NZ * NC * (CAP + 1)].reshape(NC, NX, NX, NZ, NC)
    blocks = lax.dynamic_slice(blocks, (0, 0, x, 0, c, 0), (NC, NX, 1, NZ, 1, CAP))
    counts = lax.dynamic_slice(counts, (0, 0, x, 0, c), (NC, NX, 1, NZ, 1))
    blocks = blocks.reshape(NC, NX, NZ, CAP)
    counts = counts.reshape(NC, NX, NZ, 1)
    shape = (NC, NX, NZ, CAP)
    dc, dx, zo, k = (lax.broadcasted_iota(jnp.int32, shape, i) for i in range(4))
    xs, cs = (x - dx) % NX, c ^ dc
    tile = zo * (PART * CAP) + xs * (NC * CAP) + cs * CAP + k
    link = (dc * NX + dx) * LB + blocks
    positions = lax.broadcasted_iota(jnp.int32, (TILES, TILES), 1)
    live = (k < counts).reshape(TILES)
    pad = TILES + ZERO_LINK * 512
    code = (tile + link * 512).reshape(TILES, 1) - pad
    before = positions < lax.broadcasted_iota(jnp.int32, (TILES, TILES), 0)
    rank = jnp.sum(jnp.where(before & live[None, :], 1, 0), axis=1, keepdims=True)
    target = lax.broadcasted_iota(jnp.int32, (TILES, SLOTS), 1)
    hit = (rank == target) & live[:, None]
    codes = jnp.sum(jnp.where(hit, code, 0), axis=0) + pad
    return jnp.sum(live.astype(jnp.int32)).reshape(1), codes


def body(
    link_flow,
    free_time,
    capacity,
    demand,
    path_od,
    send_blocks,
    send_counts,
    tile_links,
    tile_paths,
):
    x, z, c = lax.axis_index("x"), lax.axis_index("z"), lax.axis_index("c")
    rows = PART * CAP * HOPS
    links = tile_links[0].reshape(NX, NZ, NC * CAP * HOPS, BLK)
    links = jnp.transpose(links, (1, 0, 2, 3)).reshape(NZ, rows, BLK)
    paths = jnp.transpose(tile_paths[0].reshape(NX, NZ, NC * CAP), (1, 0, 2))
    paths = jnp.pad(paths.reshape(NZ, 1, PART * CAP), ((0, 0), (0, 7), (0, BLK - PART * CAP)))
    payload = jnp.concatenate([links, paths], axis=1)
    payload = lax.all_to_all(payload, "z", split_axis=0, concat_axis=0, tiled=True)
    tiles = payload[:, :rows].reshape(TILES, HOPS, BLK).astype(jnp.float32)
    ahead = (lax.broadcasted_iota(jnp.int32, (NZ, PART * CAP), 0) - z) % NZ
    names = (ahead * PB + payload[:, rows, : PART * CAP]).reshape(TILES)
    names = jnp.concatenate([names, jnp.full((8,), ZERO_PATH, jnp.int32)])

    info = jnp.concatenate([send_blocks[0].reshape(-1), send_counts[0].reshape(-1)])
    info = info.astype(jnp.float32)
    info_size = info.shape[0]
    info = jnp.pad(info, (0, Q * BLK - info_size)).reshape(1, Q, BLK)
    free = free_time.reshape(LB, 1, BLK)
    room = capacity.reshape(LB, 1, BLK)
    current = jnp.transpose(link_flow.reshape(Q, LB, BLK), (1, 0, 2))
    od = path_od
    demands = demand[:, 0, :]
    count = codes = wide = None
    for iteration in range(ITERS):
        times = bpr_times(current, free, room)
        if iteration == 0:
            times = jnp.concatenate([times, info], axis=0)
        if iteration == 0:
            row = lax.all_gather(times, "x")
            mine = [times] + [row[(x - d) % NX] for d in range(1, NX)]
        else:
            mine = [times] + [shift(times, "x", NX, d) for d in range(1, NX)]
        other = shift(jnp.concatenate(mine, axis=0), "c", NC, 1)
        stride = times.shape[0]
        if iteration == 0:
            infos = [m[LB] for m in mine] + [other[d * stride + LB] for d in range(NX)]
            infos = jnp.stack([v.reshape(-1)[:info_size] for v in infos])
            count, codes = live_list(infos.astype(jnp.int32), x, c)
        segments = [(d, 0, LB) for d in range(NX)] + [(NX, d * stride, LB) for d in range(NX)]
        partials = tile_call(
            count, codes, names, tiles, mine + [other], segments, [PB] * NZ, True
        )
        partials = [partials[0]] + [shift(partials[d], "z", NZ, d) for d in range(1, NZ)]
        flow, wide = logit_call(od, demands, partials)
        flows = [flow] + [shift(flow, "z", NZ, -d) for d in range(1, NZ)]
        segments = [(d, 0, PB) for d in range(NZ)]
        loads = tile_call(
            count, codes, names, tiles, flows, segments, [LB] * NX + [NX * LB], False
        )
        given = shift(loads[NX], "c", NC, 1)
        sums = [loads[d] + given[d * LB : (d + 1) * LB] for d in range(NX)]
        auxiliary = sums[0]
        for d in range(1, NX):
            auxiliary = auxiliary + shift(sums[d], "x", NX, -d)
        current = current + (auxiliary - current) / (iteration + 2.0)
    final_times = jnp.sum(bpr_times(current, free, room), axis=1).reshape(LB * BLK)
    groups = lax.axis_size("ens")
    final_times = final_times.reshape(LB, BLK)
    total, reach = final_times, 1
    while reach < groups:
        pairs = [(n, n ^ reach) for n in range(groups)]
        total = total + lax.ppermute(total, "ens", pairs)
        reach *= 2
    mean_time = total.reshape(LB * BLK) / (Q * groups)
    return (jnp.transpose(current, (1, 0, 2)).reshape(Q, LB * BLK), wide, mean_time)


def solution(mesh):
    fine = Mesh(
        np.asarray(mesh.devices).reshape(NX, NZ, NC, -1), ("x", "z", "c", "ens")
    )
    dom = ("x", "z", "c")
    in_specs = (
        P("ens", dom),
        P(dom),
        P(dom),
        P("ens", dom, None),
        P(dom, None),
        P(dom, None, None),
        P(dom, None),
        P(dom, None, None, None, None),
        P(dom, None, None),
    )
    out_specs = (P("ens", dom), P("ens", dom), P(dom))
    return jax.shard_map(body, mesh=fine, in_specs=in_specs, out_specs=out_specs, check_vma=False)
```
